32 devices in a mesh: rows: 8 (over z, x), head: 4 (over y, core).
Axes of the slice: x: 2, y: 2, z: 4, core: 2. Of those that a mesh axis runs over, the one named last changes fastest.
Arguments:
- inputs: bfloat16 [2, 32, 512, 768], P(None, ('rows', 'head')), may hold values from -6 to 6
- qkv_weight: bfloat16 [768, 2304], P('rows', 'head'), may hold values from -0.3125 to 0.3125
- out_weight: bfloat16 [768, 768], P('rows', 'head'), may hold values from -0.625 to 0.625
- up_weight: bfloat16 [768, 3072], P('rows', 'head'), may hold values from -0.21875 to 0.21875
- down_weight: bfloat16 [3072, 768], P('rows', 'head'), may hold values from -0.109375 to 0.109375
- biases: bfloat16 [8, 768], P('head', 'rows'), may hold values from -1.1953125 to 1.1953125
- norm_params: bfloat16 [4, 768], P('head', 'rows'), may hold values from -0.6 to 1.65
- cotangent: bfloat16 [2, 32, 512, 768], P(None, ('rows', 'head')), may hold values from -6 to 6
- boundaries: int32 [2, 32], P(None, 'rows'), may hold values from 1 to 511, as said below
- lengths: int32 [2, 32], P(None, 'rows'), may hold values from 257 to 512, as said below
Outputs:
- output: bfloat16 [2, 32, 512, 768], P(None, ('rows', 'head'))
- input_grad: float32 [2, 32, 512, 768], P(None, ('rows', 'head'))
- qkv_grad: float32 [768, 2304], P('rows', 'head')
- out_grad: float32 [768, 768], P('rows', 'head')
- up_grad: float32 [768, 3072], P('rows', 'head')
- down_grad: float32 [3072, 768], P('rows', 'head')
- bias_grad: float32 [8, 768], P('head', 'rows')
- norm_grad: float32 [4, 768], P('head', 'rows')
The draws below stay inside these ranges and needn't reach their ends.
Inputs may be any that keep to these rules, and one draw needn't show every extreme that they name: `boundaries`: each row's boundary lies below its own length, so both sentences of a row hold tokens. `lengths`: every length exceeds half of 512.
All inputs are finite; a program needn't handle non-finite values.
Results may differ from the reference program's by a relative error of at most 0.017.
The reference program's roundings to bfloat16 on the way count: a program that leaves them out, or rounds other values in their place, can miss the bound.
Values may be sent and summed in bfloat16 or wider, within the bound.
A program may use at most 192 MiB of HBM per device.

```python
import math
import jax
import jax.numpy as jnp
from jax import lax

D = 768
HEADS = 12
HD = 64
FF = 3072
SEQ = 512
MICRO = 2
SEQS = 32


def lengths_and_bounds(key):
    base_key = jax.random.fold_in(key, 17)
    key_cut, key_bound = jax.random.split(base_key)
    cut_amount = jax.random.randint(key_cut, (MICRO, SEQS), -(SEQ // 4), SEQ // 2)
    length_rows = SEQ - jnp.maximum(cut_amount, 0)
    length_rows = length_rows.at[0, 0].set(SEQ // 2 + 1).at[0, 1].set(SEQ)
    bound_rows = jax.random.randint(key_bound, (MICRO, SEQS), 1, length_rows)
    bound_rows = bound_rows.at[0, 0].set(1).at[0, 1].set(SEQ - 1)
    return (length_rows.astype(jnp.int32), bound_rows.astype(jnp.int32))


def draw_lengths(key, part):
    return lengths_and_bounds(key)[0]


def draw_boundaries(key, part):
    return lengths_and_bounds(key)[1]


def draw_norm_params(key, part):
    key_gain, key_shift = jax.random.split(jax.random.fold_in(key, 29))
    gain_rows = jnp.exp(jax.random.uniform(key_gain, (2, D), jnp.float32, -0.5, 0.5))
    shift_rows = jax.random.uniform(key_shift, (2, D), jnp.float32, -0.6, 0.6)
    return jnp.stack([gain_rows[0], shift_rows[0], gain_rows[1], shift_rows[1]]).astype(jnp.bfloat16)


def block_scale(own_key, dims, shards, smallest, high):
    def one(position, parts):
        draws = jax.random.uniform(jax.random.fold_in(jax.random.fold_in(own_key, 6), position), (parts,), jnp.float32, smallest / len(shards), high / len(shards))
        return jnp.repeat(jnp.exp(draws), dims[position] // parts).reshape((-1,) + (1,) * (len(dims) - position - 1))

    level = one(*shards[0])
    for cut in shards[1:]:
        level = level * one(*cut)
    return level


def normal_values(rng, extent, spread, reach, cuts=(), kind=jnp.bfloat16):
    array = jax.random.normal(rng, extent, jnp.float32) * spread
    if len(cuts) > 0:
        array = block_scale(rng, extent, cuts, -0.22, 0.18) * array
    return jnp.clip(array, min=-reach, max=reach).astype(kind)


def setup_inputs(seed: int = 0) -> dict:
    splits = jax.random.split(jax.random.key(seed), 11)
    return {
        "inputs": normal_values(splits[0], (MICRO, SEQS, SEQ, D), 1.0, 6.0, ((1, 32),)),
        "qkv_weight": normal_values(splits[1], (D, 3 * D), (D // 2) ** -0.5, 0.3125, ((0, 8), (1, 4))),
        "out_weight": normal_values(splits[2], (D, D), (D // 8) ** -0.5, 0.625, ((0, 8), (1, 4))),
        "up_weight": normal_values(splits[3], (D, FF), D ** -0.5, 0.21875, ((0, 8), (1, 4))),
        "down_weight": normal_values(splits[4], (FF, D), FF ** -0.5, 0.109375, ((0, 8), (1, 4))),
        "biases": normal_values(splits[5], (8, D), 0.3, 1.1953125, ((0, 4), (1, 8))),
        "norm_params": draw_norm_params(jax.random.fold_in(splits[10], 71), 0),
        "cotangent": normal_values(splits[7], (MICRO, SEQS, SEQ, D), 1.0, 6.0, ((1, 32),)),
        "boundaries": draw_boundaries(jax.random.fold_in(splits[10], 71), 0),
        "lengths": draw_lengths(jax.random.fold_in(splits[10], 71), 0),
    }


@jax.custom_vjp
def low(v):
    return lax.optimization_barrier(v.astype(jnp.bfloat16)).astype(jnp.float32)

@jax.custom_vjp
def low_back(v):
    return v

def low_keep(v):
    return (low(v), None)

def low_pass(kept, grad):
    return (grad,)

def back_keep(v):
    return (v, None)

def back_low(kept, grad):
    return (low(grad),)
low.defvjp(low_keep, low_pass)
low_back.defvjp(back_keep, back_low)
EPSILON = 1e-06
HIGHEST = lax.Precision.HIGHEST

def layer_norm(values_in, gain_row, shift_row):
    average = lax.optimization_barrier(jnp.mean(values_in, axis=-1, keepdims=True))
    centered = values_in - average
    variance = lax.optimization_barrier(jnp.mean(centered * centered, axis=-1, keepdims=True))
    return centered * lax.rsqrt(variance + EPSILON) * gain_row + shift_row

def layer_forward(block_in, qkv_weight, out_weight, up_weight, down_weight, biases, norm_params, bounds, lengths):
    seq_count = block_in.shape[0]
    zero_part = jnp.zeros((HEADS, HD), jnp.float32)
    head_bias = jnp.stack([biases[0].reshape(HEADS, HD), zero_part, biases[1].reshape(HEADS, HD)], axis=1).reshape(3 * D)
    project = jnp.einsum('gsd,de->gse', block_in, qkv_weight, precision=HIGHEST) + head_bias
    project = low_back(low(project)).reshape(seq_count, SEQ, HEADS, 3, HD)
    scale_factor = HD ** (-0.5)
    scores = low_back(jnp.einsum('gqhe,gkhe->ghqk', project[:, :, :, 0], project[:, :, :, 1], precision=HIGHEST) * scale_factor)
    positions = jnp.arange(SEQ, dtype=jnp.int32)
    segment = positions[None, :] >= bounds[:, None]
    allowed = (segment[:, :, None] == segment[:, None, :]) & (positions[None, None, :] < lengths[:, None, None])
    masked = jnp.where(allowed[:, None], scores, -1e+30)
    weights_low = low(jax.nn.softmax(masked, axis=-1))
    context = jnp.einsum('ghqk,gkhe->gqhe', weights_low, project[:, :, :, 2], precision=HIGHEST).reshape(seq_count, SEQ, D)
    context = low_back(low(context))
    attended = low_back(jnp.einsum('gsd,de->gse', context, out_weight, precision=HIGHEST)) + biases[2]
    hidden = layer_norm(block_in + attended, norm_params[0], norm_params[1])
    inner_pre = low_back(jnp.einsum('gsd,df->gsf', low(hidden), up_weight, precision=HIGHEST)) + biases[4:8].reshape(FF)
    active = low(jax.nn.gelu(inner_pre, approximate=False))
    outer_out = low_back(jnp.einsum('gsf,fd->gsd', active, down_weight, precision=HIGHEST)) + biases[3]
    return layer_norm(hidden + outer_out, norm_params[2], norm_params[3])

def reference(inputs, qkv_weight, out_weight, up_weight, down_weight, biases, norm_params, cotangent, boundaries, lengths):
    seq_count = MICRO * SEQS
    group_size = math.gcd(seq_count, max(1, 4096 // SEQ))
    blocks = seq_count // group_size
    params = (qkv_weight.astype(jnp.float32), out_weight.astype(jnp.float32), up_weight.astype(jnp.float32), down_weight.astype(jnp.float32), biases.astype(jnp.float32), norm_params.astype(jnp.float32))
    block_in = inputs.astype(jnp.float32).reshape(blocks, group_size, SEQ, D)
    block_cot = cotangent.astype(jnp.float32).reshape(blocks, group_size, SEQ, D)
    block_bounds = boundaries.reshape(blocks, group_size)
    block_lengths = lengths.reshape(blocks, group_size)

    def one_block(totals, pieces):
        piece_in, piece_cot, piece_bounds, piece_lengths = pieces

        def forward(values_in, qkv_float, out_float, up_float, down_float, bias_float, norm_float):
            return layer_forward(values_in, qkv_float, out_float, up_float, down_float, bias_float, norm_float, piece_bounds, piece_lengths)
        result, pullback = jax.vjp(forward, piece_in, params[0], params[1], params[2], params[3], params[4], params[5])
        gradients = pullback(piece_cot)
        totals = tuple((total_now + grad_now for total_now, grad_now in zip(totals, gradients[1:])))
        return (totals, (result.astype(jnp.bfloat16), gradients[0]))
    starting = tuple((jnp.zeros(param_now.shape, jnp.float32) for param_now in params))
    totals, (results, in_grads) = lax.scan(one_block, starting, (block_in, block_cot, block_bounds, block_lengths))
    return (results.reshape(MICRO, SEQS, SEQ, D), in_grads.reshape(MICRO, SEQS, SEQ, D), totals[0], totals[1], totals[2], totals[3], totals[4], totals[5])
```

```python
import jax
import jax.numpy as jnp
from jax import lax
from jax.sharding import PartitionSpec as P

HD = 64
EPSILON = 1e-06
ROOT_HALF = 0.7071067811865476
INVERSE_ROOT_TWO_PI = 0.3989422804014327
AXES = ("rows", "head")


def contract_rows(left, right):
    return lax.dot_general(
        left, right, (((0,), (0,)), ((), ())), preferred_element_type=jnp.float32
    )


def contract_cols(left, right):
    return lax.dot_general(
        left, right, (((1,), (1,)), ((), ())), preferred_element_type=jnp.float32
    )


def norm_forward(values_in, gain_row, shift_row):
    average = jnp.mean(values_in, axis=-1, keepdims=True)
    centered = values_in - average
    variance = jnp.mean(centered * centered, axis=-1, keepdims=True)
    inverse_scale = lax.rsqrt(variance + EPSILON)
    normed = centered * inverse_scale
    return (normed * gain_row + shift_row, normed, inverse_scale)


def norm_backward(grad_out, normed, inverse_scale, gain_row):
    grad_normed = grad_out * gain_row
    first_mean = jnp.mean(grad_normed, axis=-1, keepdims=True)
    second_mean = jnp.mean(grad_normed * normed, axis=-1, keepdims=True)
    grad_in = inverse_scale * (grad_normed - first_mean - normed * second_mean)
    return (grad_in, jnp.sum(grad_out * normed, axis=0), jnp.sum(grad_out, axis=0))


def masked_scores(queries, keys_in, bound, length):
    seq = queries.shape[0]
    positions = lax.broadcasted_iota(jnp.int32, (seq,), 0)
    segment = positions >= bound
    allowed = (segment[:, None] == segment[None, :]) & (positions[None, :] < length)
    scores = jnp.einsum(
        "qhe,khe->hqk", queries, keys_in, preferred_element_type=jnp.float32
    ) * HD ** (-0.5)
    return jnp.where(allowed[None], scores, -1e30)


def attend_forward(queries, keys_in, values_in, bound, length):
    scores = masked_scores(queries, keys_in, bound, length)
    highest = jnp.max(scores, axis=-1, keepdims=True)
    raised = jnp.exp(scores - highest)
    totals = jnp.sum(raised, axis=-1, keepdims=True)
    weights_low = (raised / totals).astype(jnp.bfloat16)
    context = jnp.einsum("hqk,khe->qhe", weights_low, values_in, preferred_element_type=jnp.float32)
    log_total = (highest + jnp.log(totals))[..., 0]
    return (context.astype(jnp.bfloat16), log_total)


def attend_backward(queries, keys_in, values_in, bound, length, log_total, grad_context):
    scores = masked_scores(queries, keys_in, bound, length)
    weights_full = jnp.exp(scores - log_total[..., None])
    weights_low = weights_full.astype(jnp.bfloat16)
    grad_values = jnp.einsum(
        "hqk,qhe->khe", weights_low, grad_context, preferred_element_type=jnp.float32
    )
    grad_weights = jnp.einsum(
        "qhe,khe->hqk", grad_context, values_in, preferred_element_type=jnp.float32
    )
    inner_sum = jnp.sum(weights_full * grad_weights, axis=-1, keepdims=True)
    grad_scores = (weights_full * (grad_weights - inner_sum)).astype(jnp.bfloat16)
    grad_queries = jnp.einsum(
        "hqk,khe->qhe", grad_scores, keys_in, preferred_element_type=jnp.float32
    ) * HD ** (-0.5)
    grad_keys = jnp.einsum(
        "hqk,qhe->khe", grad_scores, queries, preferred_element_type=jnp.float32
    ) * HD ** (-0.5)
    return jnp.stack([grad_queries, grad_keys, grad_values], axis=2).astype(jnp.bfloat16)


def gather(shard, row_axis):
    rows, head = lax.axis_size("rows"), lax.axis_size("head")
    a, b = shard.shape
    every = lax.all_gather(shard, AXES, axis=0, tiled=False).reshape(rows, head, a, b)
    if row_axis == 0:
        return every.transpose(0, 2, 1, 3).reshape(rows * a, head * b)
    return every.transpose(1, 2, 0, 3).reshape(head * a, rows * b)


def scatter(grad, row_axis):
    rows, head = lax.axis_size("rows"), lax.axis_size("head")
    a, b = grad.shape
    if row_axis == 0:
        parts = grad.reshape(rows, a // rows, head, b // head).transpose(0, 2, 1, 3)
    else:
        parts = grad.reshape(head, a // head, rows, b // rows).transpose(2, 0, 1, 3)
    parts = parts.reshape((rows * head,) + parts.shape[2:]).astype(jnp.bfloat16)
    return lax.psum_scatter(parts, AXES, scatter_dimension=0, tiled=False).astype(jnp.float32)


def shards(
    inputs,
    qkv_weight,
    out_weight,
    up_weight,
    down_weight,
    biases,
    norm_params,
    cotangent,
    boundaries,
    lengths,
):
    micro, seq_per, seq, width = inputs.shape
    count = micro * seq_per
    heads = width // HD
    qkv_full, out_full, up_full, down_full = (
        gather(w, 0) for w in (qkv_weight, out_weight, up_weight, down_weight)
    )
    bias_float = gather(biases, 1).astype(jnp.float32)
    norm_float = gather(norm_params, 1).astype(jnp.float32)
    first_seq = lax.axis_index("head") * seq_per
    bounds = lax.dynamic_slice_in_dim(boundaries, first_seq, seq_per, 1).reshape(count)
    lens = lax.dynamic_slice_in_dim(lengths, first_seq, seq_per, 1).reshape(count)

    tokens = inputs.reshape(count * seq, width)
    zero_part = jnp.zeros((heads, HD), jnp.float32)
    head_bias = jnp.stack(
        [bias_float[0].reshape(heads, HD), zero_part, bias_float[1].reshape(heads, HD)], axis=1
    ).reshape(3 * width)
    project = (jnp.dot(tokens, qkv_full, preferred_element_type=jnp.float32) + head_bias).astype(
        jnp.bfloat16
    )
    items = project.reshape(count, seq, heads, 3, HD)
    q, k, v = items[:, :, :, 0], items[:, :, :, 1], items[:, :, :, 2]
    context, log_total = jax.vmap(attend_forward)(q, k, v, bounds, lens)
    context = context.reshape(count * seq, width)
    attended = jnp.dot(context, out_full, preferred_element_type=jnp.float32) + bias_float[2]
    hidden, normed_one, scale_one = norm_forward(
        tokens.astype(jnp.float32) + attended, norm_float[0], norm_float[1]
    )
    hidden_low = hidden.astype(jnp.bfloat16)
    inner_pre = jnp.dot(hidden_low, up_full, preferred_element_type=jnp.float32) + bias_float[
        4:8
    ].reshape(-1)
    cdf = 0.5 * (1.0 + lax.erf(inner_pre * ROOT_HALF))
    active_low = (inner_pre * cdf).astype(jnp.bfloat16)
    slope = cdf + inner_pre * jnp.exp(-0.5 * inner_pre * inner_pre) * INVERSE_ROOT_TWO_PI
    outer_out = jnp.dot(active_low, down_full, preferred_element_type=jnp.float32) + bias_float[3]
    output_float, normed_two, scale_two = norm_forward(
        hidden + outer_out, norm_float[2], norm_float[3]
    )
    grad_out = cotangent.reshape(count * seq, width).astype(jnp.float32)
    grad_two, gain_two, shift_two = norm_backward(grad_out, normed_two, scale_two, norm_float[2])
    grad_two_low = grad_two.astype(jnp.bfloat16)
    down_grad = scatter(contract_rows(active_low, grad_two_low), 0)
    grad_inner = contract_cols(grad_two_low, down_full) * slope
    grad_inner_low = grad_inner.astype(jnp.bfloat16)
    up_grad = scatter(contract_rows(hidden_low, grad_inner_low), 0)
    grad_hidden = contract_cols(grad_inner_low, up_full) + grad_two
    grad_one, gain_one, shift_one = norm_backward(grad_hidden, normed_one, scale_one, norm_float[0])
    grad_one_low = grad_one.astype(jnp.bfloat16)
    out_grad = scatter(contract_rows(context, grad_one_low), 0)
    grad_context = contract_cols(grad_one_low, out_full).astype(jnp.bfloat16)
    grad_items = grad_context.reshape(count, seq, heads, HD)
    grad_project = jax.vmap(attend_backward)(q, k, v, bounds, lens, log_total, grad_items)
    grad_project = grad_project.reshape(count * seq, 3 * width)
    qkv_grad = scatter(contract_rows(tokens, grad_project), 0)
    grad_input = contract_cols(grad_project, qkv_full) + grad_one
    project_sums = jnp.sum(grad_project, axis=0, dtype=jnp.float32).reshape(heads, 3, HD)
    bias_grad = jnp.concatenate(
        [
            project_sums[:, 0].reshape(1, width),
            project_sums[:, 2].reshape(1, width),
            jnp.sum(grad_one, axis=0).reshape(1, width),
            jnp.sum(grad_two, axis=0).reshape(1, width),
            jnp.sum(grad_inner, axis=0).reshape(4, width),
        ],
        axis=0,
    )
    norm_grad = jnp.stack([gain_one, shift_one, gain_two, shift_two])
    return (
        output_float.astype(jnp.bfloat16).reshape(inputs.shape),
        grad_input.reshape(inputs.shape),
        qkv_grad,
        out_grad,
        up_grad,
        down_grad,
        scatter(bias_grad, 1),
        scatter(norm_grad, 1),
    )


def solution(mesh):
    tokens = P(None, ("rows", "head"), None, None)
    weight = P("rows", "head")
    small = P("head", "rows")
    per_row = P(None, "rows")
    return jax.shard_map(
        shards,
        mesh=mesh,
        in_specs=(tokens, weight, weight, weight, weight, small, small, tokens, per_row, per_row),
        out_specs=(tokens, tokens, weight, weight, weight, weight, small, small),
        check_vma=False,
    )
```

```python
import functools

import jax
import jax.numpy as jnp
from jax import lax
from jax.experimental import pallas as pl
from jax.experimental.pallas import tpu as pltpu
from jax.sharding import PartitionSpec as P

HD = 64
EPSILON = 1e-06
ROOT_HALF = 0.7071067811865476
INVERSE_ROOT_TWO_PI = 0.3989422804014327
AXES = ("rows", "head")


def contract_rows(left, right):
    return lax.dot_general(
        left, right, (((0,), (0,)), ((), ())), preferred_element_type=jnp.float32
    )


def contract_cols(left, right):
    return lax.dot_general(
        left, right, (((1,), (1,)), ((), ())), preferred_element_type=jnp.float32
    )


def norm_forward(values_in, gain_row, shift_row):
    average = jnp.mean(values_in, axis=-1, keepdims=True)
    centered = values_in - average
    variance = jnp.mean(centered * centered, axis=-1, keepdims=True)
    inverse_scale = lax.rsqrt(variance + EPSILON)
    normed = centered * inverse_scale
    return (normed * gain_row + shift_row, normed, inverse_scale)


def norm_backward(grad_out, normed, inverse_scale, gain_row):
    grad_normed = grad_out * gain_row
    first_mean = jnp.mean(grad_normed, axis=-1, keepdims=True)
    second_mean = jnp.mean(grad_normed * normed, axis=-1, keepdims=True)
    grad_in = inverse_scale * (grad_normed - first_mean - normed * second_mean)
    return (grad_in, jnp.sum(grad_out * normed, axis=0), jnp.sum(grad_out, axis=0))


def masked_scores(queries, keys_in, bound, length):
    seq = queries.shape[0]
    positions = lax.broadcasted_iota(jnp.int32, (seq,), 0)
    segment = positions >= bound
    allowed = (segment[:, None] == segment[None, :]) & (positions[None, :] < length)
    scores = jnp.einsum(
        "qhe,khe->hqk", queries, keys_in, preferred_element_type=jnp.float32
    ) * HD ** (-0.5)
    return jnp.where(allowed[None], scores, -1e30)


def attend_forward(queries, keys_in, values_in, bound, length):
    scores = masked_scores(queries, keys_in, bound, length)
    highest = jnp.max(scores, axis=-1, keepdims=True)
    raised = jnp.exp(scores - highest)
    totals = jnp.sum(raised, axis=-1, keepdims=True)
    weights_low = (raised / totals).astype(jnp.bfloat16)
    context = jnp.einsum("hqk,khe->qhe", weights_low, values_in, preferred_element_type=jnp.float32)
    log_total = (highest + jnp.log(totals))[..., 0]
    return (context.astype(jnp.bfloat16), log_total)


def attend_backward(queries, keys_in, values_in, bound, length, log_total, grad_context):
    scores = masked_scores(queries, keys_in, bound, length)
    weights_full = jnp.exp(scores - log_total[..., None])
    weights_low = weights_full.astype(jnp.bfloat16)
    grad_values = jnp.einsum(
        "hqk,qhe->khe", weights_low, grad_context, preferred_element_type=jnp.float32
    )
    grad_weights = jnp.einsum(
        "qhe,khe->hqk", grad_context, values_in, preferred_element_type=jnp.float32
    )
    inner_sum = jnp.sum(weights_full * grad_weights, axis=-1, keepdims=True)
    grad_scores = (weights_full * (grad_weights - inner_sum)).astype(jnp.bfloat16)
    grad_queries = jnp.einsum(
        "hqk,khe->qhe", grad_scores, keys_in, preferred_element_type=jnp.float32
    ) * HD ** (-0.5)
    grad_keys = jnp.einsum(
        "hqk,qhe->khe", grad_scores, queries, preferred_element_type=jnp.float32
    ) * HD ** (-0.5)
    return jnp.stack([grad_queries, grad_keys, grad_values], axis=2).astype(jnp.bfloat16)


def gather(shard, row_axis):
    rows, head = lax.axis_size("rows"), lax.axis_size("head")
    a, b = shard.shape
    every = lax.all_gather(shard, AXES, axis=0, tiled=False).reshape(rows, head, a, b)
    if row_axis == 0:
        return every.transpose(0, 2, 1, 3).reshape(rows * a, head * b)
    return every.transpose(1, 2, 0, 3).reshape(head * a, rows * b)


def scatter(grad, row_axis):
    rows, head = lax.axis_size("rows"), lax.axis_size("head")
    a, b = grad.shape
    if row_axis == 0:
        parts = grad.reshape(rows, a // rows, head, b // head).transpose(0, 2, 1, 3)
    else:
        parts = grad.reshape(head, a // head, rows, b // rows).transpose(2, 0, 1, 3)
    parts = parts.reshape((rows * head,) + parts.shape[2:]).astype(jnp.bfloat16)
    return lax.psum_scatter(parts, AXES, scatter_dimension=0, tiled=False).astype(jnp.float32)


def shards_plain(
    inputs,
    qkv_weight,
    out_weight,
    up_weight,
    down_weight,
    biases,
    norm_params,
    cotangent,
    boundaries,
    lengths,
):
    micro, seq_per, seq, width = inputs.shape
    count = micro * seq_per
    heads = width // HD
    qkv_full, out_full, up_full, down_full = (
        gather(w, 0) for w in (qkv_weight, out_weight, up_weight, down_weight)
    )
    bias_float = gather(biases, 1).astype(jnp.float32)
    norm_float = gather(norm_params, 1).astype(jnp.float32)
    first_seq = lax.axis_index("head") * seq_per
    bounds = lax.dynamic_slice_in_dim(boundaries, first_seq, seq_per, 1).reshape(count)
    lens = lax.dynamic_slice_in_dim(lengths, first_seq, seq_per, 1).reshape(count)

    tokens = inputs.reshape(count * seq, width)
    zero_part = jnp.zeros((heads, HD), jnp.float32)
    head_bias = jnp.stack(
        [bias_float[0].reshape(heads, HD), zero_part, bias_float[1].reshape(heads, HD)], axis=1
    ).reshape(3 * width)
    project = (jnp.dot(tokens, qkv_full, preferred_element_type=jnp.float32) + head_bias).astype(
        jnp.bfloat16
    )
    items = project.reshape(count, seq, heads, 3, HD)
    q, k, v = items[:, :, :, 0], items[:, :, :, 1], items[:, :, :, 2]
    context, log_total = jax.vmap(attend_forward)(q, k, v, bounds, lens)
    context = context.reshape(count * seq, width)
    attended = jnp.dot(context, out_full, preferred_element_type=jnp.float32) + bias_float[2]
    hidden, normed_one, scale_one = norm_forward(
        tokens.astype(jnp.float32) + attended, norm_float[0], norm_float[1]
    )
    hidden_low = hidden.astype(jnp.bfloat16)
    inner_pre = jnp.dot(hidden_low, up_full, preferred_element_type=jnp.float32) + bias_float[
        4:8
    ].reshape(-1)
    cdf = 0.5 * (1.0 + lax.erf(inner_pre * ROOT_HALF))
    active_low = (inner_pre * cdf).astype(jnp.bfloat16)
    slope = cdf + inner_pre * jnp.exp(-0.5 * inner_pre * inner_pre) * INVERSE_ROOT_TWO_PI
    outer_out = jnp.dot(active_low, down_full, preferred_element_type=jnp.float32) + bias_float[3]
    output_float, normed_two, scale_two = norm_forward(
        hidden + outer_out, norm_float[2], norm_float[3]
    )
    grad_out = cotangent.reshape(count * seq, width).astype(jnp.float32)
    grad_two, gain_two, shift_two = norm_backward(grad_out, normed_two, scale_two, norm_float[2])
    grad_two_low = grad_two.astype(jnp.bfloat16)
    down_grad = scatter(contract_rows(active_low, grad_two_low), 0)
    grad_inner = contract_cols(grad_two_low, down_full) * slope
    grad_inner_low = grad_inner.astype(jnp.bfloat16)
    up_grad = scatter(contract_rows(hidden_low, grad_inner_low), 0)
    grad_hidden = contract_cols(grad_inner_low, up_full) + grad_two
    grad_one, gain_one, shift_one = norm_backward(grad_hidden, normed_one, scale_one, norm_float[0])
    grad_one_low = grad_one.astype(jnp.bfloat16)
    out_grad = scatter(contract_rows(context, grad_one_low), 0)
    grad_context = contract_cols(grad_one_low, out_full).astype(jnp.bfloat16)
    grad_items = grad_context.reshape(count, seq, heads, HD)
    grad_project = jax.vmap(attend_backward)(q, k, v, bounds, lens, log_total, grad_items)
    grad_project = grad_project.reshape(count * seq, 3 * width)
    qkv_grad = scatter(contract_rows(tokens, grad_project), 0)
    grad_input = contract_cols(grad_project, qkv_full) + grad_one
    project_sums = jnp.sum(grad_project, axis=0, dtype=jnp.float32).reshape(heads, 3, HD)
    bias_grad = jnp.concatenate(
        [
            project_sums[:, 0].reshape(1, width),
            project_sums[:, 2].reshape(1, width),
            jnp.sum(grad_one, axis=0).reshape(1, width),
            jnp.sum(grad_two, axis=0).reshape(1, width),
            jnp.sum(grad_inner, axis=0).reshape(4, width),
        ],
        axis=0,
    )
    norm_grad = jnp.stack([gain_one, shift_one, gain_two, shift_two])
    return (
        output_float.astype(jnp.bfloat16).reshape(inputs.shape),
        grad_input.reshape(inputs.shape),
        qkv_grad,
        out_grad,
        up_grad,
        down_grad,
        scatter(bias_grad, 1),
        scatter(norm_grad, 1),
    )


MESH = pl.DeviceIdType.MESH
NZ, NX, NY, NC = 4, 2, 2, 2
FIRST = ("x", "x", "y", "y", "x")


def spot():
    r, h = lax.axis_index("rows"), lax.axis_index("head")
    return r // NX, lax.rem(r, NX), h // NC, lax.rem(h, NC)


def dev(z, x, y, c):
    return (z * NX + x, y * NC + c)


def other_z(z, d):
    return lax.rem(z + d, NZ)


def meet(z, x, y, c):
    barrier = pltpu.get_barrier_semaphore()
    mates = [dev(other_z(z, d), x, y, c) for d in range(1, NZ)]
    mates += [dev(z, 1 - x, y, c), dev(z, x, 1 - y, c), dev(z, x, y, 1 - c)]
    for mate in mates:
        pl.semaphore_signal(barrier, inc=1, device_id=mate, device_id_type=MESH)
    pl.semaphore_wait(barrier, len(mates))


def tile(w, ref, z, x, y, c):
    r, h = dev(z, x, y, c)
    if w == 2:
        return ref.at[pl.ds(pl.multiple_of(r * 96, 32), 96), pl.ds(pl.multiple_of(h * 768, 128), 768)]
    if w == 3:
        return ref.at[pl.ds(pl.multiple_of(h * 192, 64), 192), pl.ds(pl.multiple_of(r * 384, 128), 384)]
    return ref.at[h, r]


class Spread:
    def __init__(self, ins, outs, send_sem, recv_sem, local_sem):
        self.ins, self.outs = ins, outs
        self.send_sem, self.recv_sem, self.local_sem = send_sem, recv_sem, local_sem
        self.at = spot()
        self.sent = {w: [] for w in range(5)}
        self.locals = []

    def push(self, w, src, shard, to):
        k = len(self.sent[w])
        copy = pltpu.make_async_remote_copy(
            src_ref=src,
            dst_ref=tile(w, self.outs[w], *shard),
            send_sem=self.send_sem.at[w, k],
            recv_sem=self.recv_sem.at[w, self.index(shard)],
            device_id=to,
            device_id_type=MESH,
        )
        copy.start()
        self.sent[w].append(copy)

    def index(self, shard):
        r, h = dev(*shard)
        return r * (NY * NC) + h

    def take(self, w, shard):
        there = tile(w, self.outs[w], *shard)
        pltpu.make_async_remote_copy(
            src_ref=there,
            dst_ref=there,
            send_sem=self.send_sem.at[w, 0],
            recv_sem=self.recv_sem.at[w, self.index(shard)],
            device_id=dev(self.at[0], self.at[1], self.at[2], 1 - self.at[3]),
            device_id_type=MESH,
        ).wait_recv()

    def spread(self, w, src, shard, kinds):
        z, x, y, c = self.at
        to = {"x": dev(z, 1 - x, y, c), "y": dev(z, x, 1 - y, c), "c": dev(z, x, y, 1 - c)}
        for kind in kinds:
            self.push(w, src, shard, to[kind])

    def open(self, w):
        z, x, y, c = self.at
        src = self.ins[w]
        for d in range(1, NZ):
            self.push(w, src, self.at, dev(other_z(z, d), x, y, c))
        second = "y" if FIRST[w] == "x" else "x"
        self.spread(w, src, self.at, (FIRST[w], second, "c"))
        local = pltpu.make_async_copy(src, tile(w, self.outs[w], *self.at), self.local_sem.at[w])
        local.start()
        self.locals.append(local)

    def near(self, w):
        z, x, y, c = self.at
        second = "y" if FIRST[w] == "x" else "x"
        for d in range(1, NZ):
            shard = (other_z(z, d), x, y, c)
            self.take(w, shard)
            self.spread(w, tile(w, self.outs[w], *shard), shard, (FIRST[w], second, "c"))

    def middle(self, w):
        z, x, y, c = self.at
        second = "y" if FIRST[w] == "x" else "x"
        for d in range(NZ):
            shard = (other_z(z, d), 1 - x, y, c) if FIRST[w] == "x" else (other_z(z, d), x, 1 - y, c)
            self.take(w, shard)
            self.spread(w, tile(w, self.outs[w], *shard), shard, (second, "c"))

    def far(self, w):
        z, x, y, c = self.at
        for e in range(2):
            for d in range(NZ):
                if FIRST[w] == "x":
                    shard = (other_z(z, d), x if e == 0 else 1 - x, 1 - y, c)
                else:
                    shard = (other_z(z, d), 1 - x, y if e == 0 else 1 - y, c)
                self.take(w, shard)
                self.spread(w, tile(w, self.outs[w], *shard), shard, ("c",))

    def core(self, w):
        z, x, y, c = self.at
        for ey in range(2):
            for ex in range(2):
                for d in range(NZ):
                    self.take(
                        w,
                        (other_z(z, d), x if ex == 0 else 1 - x, y if ey == 0 else 1 - y, 1 - c),
                    )

    def close(self):
        for local in self.locals:
            local.wait()
        for copies in self.sent.values():
            for copy in copies:
                copy.wait_send()


def gather_kernel(*refs):
    ins, outs = refs[:5], refs[5:10]
    s = Spread(ins, outs, *refs[10:])
    meet(*s.at)
    s.open(0)
    s.open(4)
    s.near(0)
    for w in (1, 2, 3):
        s.open(w)
    s.near(4)
    s.middle(0)
    s.near(1)
    s.middle(4)
    s.near(2)
    s.far(0)
    s.far(4)
    s.middle(1)
    s.near(3)
    s.middle(2)
    s.far(1)
    s.middle(3)
    s.far(2)
    s.far(3)
    for w in range(5):
        s.core(w)
    s.close()


GATHERED = ((4, 8, 96, 576), (4, 8, 96, 192), (768, 3072), (768, 3072), (4, 8, 8, 128))


def gather_all(qkv, out, up, down_t, small):
    return pl.pallas_call(
        gather_kernel,
        out_shape=[
            jax.ShapeDtypeStruct(shape, jnp.float32 if i == 4 else jnp.bfloat16)
            for i, shape in enumerate(GATHERED)
        ],
        in_specs=[pl.BlockSpec(memory_space=pltpu.VMEM)] * 5,
        out_specs=[pl.BlockSpec(memory_space=pl.ANY)] * 5,
        scratch_shapes=[
            pltpu.SemaphoreType.DMA((5, 31)),
            pltpu.SemaphoreType.DMA((5, 32)),
            pltpu.SemaphoreType.DMA((5,)),
        ],
        compiler_params=pltpu.CompilerParams(collective_id=0, has_side_effects=True),
        name="gather_weights",
    )(qkv, out, up, down_t, small)


SHARD = ((96, 576), (96, 192), (96, 768), (192, 384), (8, 128))


def kind_of(w):
    return jnp.float32 if w == 4 else jnp.bfloat16


class Reduce:
    def __init__(self, acc, from_core, from_second, from_first, from_z, send_sem, recv_sem):
        self.acc = acc
        self.slots = (from_core, from_second, from_first, from_z)
        self.send_sem, self.recv_sem = send_sem, recv_sem
        self.at = spot()

    def shard(self, w, d, e1, e2, ec):
        z, x, y, c = self.at
        flip = lambda v, e: v + e * (1 - 2 * v)
        ex, ey = (e1, e2) if FIRST[w] == "x" else (e2, e1)
        return (other_z(z, d), flip(x, ex), flip(y, ey), flip(c, ec))

    def order(self, stage, k):
        if stage == 0:
            return (lax.rem(k, 4), 1 - lax.rem(k // 4, 2), 1 - k // 8)
        if stage == 1:
            return (lax.rem(k, 4), 1 - k // 4, 0)
        return (lax.rem(k + 1, 4), 0, 0)

    def slot(self, w, stage, shard):
        z, x, y, c = shard
        first, second = (x, y) if FIRST[w] == "x" else (y, x)
        if stage == 0:
            return (z * 2 + first) * 2 + second
        if stage == 1:
            return z * 2 + first
        return z

    def sending(self, w, stage, k):
        z, x, y, c = self.at
        if stage == 0:
            shard = self.shard(w, lax.rem(k, 4), 1 - lax.rem(k // 4, 2), 1 - k // 8, 1)
            to, place, base = dev(z, x, y, 1 - c), self.slot(w, 0, shard), 0
        elif stage == 1:
            shard = self.shard(w, lax.rem(k, 4), 1 - k // 4, 1, 0)
            to = dev(z, x, 1 - y, c) if FIRST[w] == "x" else dev(z, 1 - x, y, c)
            place, base = self.slot(w, 1, shard), 16
        elif stage == 2:
            shard = self.shard(w, lax.rem(k + 1, 4), 1, 0, 0)
            to = dev(z, 1 - x, y, c) if FIRST[w] == "x" else dev(z, x, 1 - y, c)
            place, base = self.slot(w, 2, shard), 24
        else:
            shard = self.shard(w, k + 1, 0, 0, 0)
            to, place, base = dev(other_z(z, k + 1), x, y, c), k, 28
        return pltpu.make_async_remote_copy(
            src_ref=tile(w, self.acc[w], *shard),
            dst_ref=self.slots[stage][w].at[place],
            send_sem=self.send_sem.at[w, base + k],
            recv_sem=self.recv_sem.at[w, base + place],
            device_id=to,
            device_id_type=MESH,
        )

    def arrive(self, w, stage, place):
        z, x, y, c = self.at
        here = self.slots[stage][w].at[place]
        base = (0, 16, 24, 28)[stage]
        pltpu.make_async_remote_copy(
            src_ref=here,
            dst_ref=here,
            send_sem=self.send_sem.at[w, base],
            recv_sem=self.recv_sem.at[w, base + place],
            device_id=dev(z, x, y, 1 - c),
            device_id_type=MESH,
        ).wait_recv()

    def open(self, w):
        def step(k, carry):
            self.sending(w, 0, k).start()
            return carry

        lax.fori_loop(0, 16, step, 0)

    def fold(self, w, stage):
        count = (16, 8, 4)[stage]
        leave = (8, 4, 3)[stage]

        def step(k, carry):
            d, e1, e2 = self.order(stage, k)
            shard = self.shard(w, d, e1, e2, 0)
            place = self.slot(w, stage, shard)
            self.arrive(w, stage, place)
            mine = tile(w, self.acc[w], *shard)
            total = mine[...].astype(jnp.float32) + self.slots[stage][w][place].astype(jnp.float32)
            mine[...] = total.astype(kind_of(w))

            @pl.when(jnp.logical_and(k >= 1, k <= leave))
            def _():
                self.sending(w, stage + 1, k - 1).start()

            return carry

        lax.fori_loop(0, count, step, 0)

    def finish(self, w, out):
        total = tile(w, self.acc[w], *self.at)[...].astype(jnp.float32)
        for k in range(3):
            self.arrive(w, 3, k)
            total = total + self.slots[3][w][k].astype(jnp.float32)
        out[...] = total

    def close(self, w):
        for stage, count in enumerate((16, 8, 4, 3)):

            def step(k, carry, stage=stage):
                self.sending(w, stage, k).wait_send()
                return carry

            lax.fori_loop(0, count, step, 0)


def reduce_scratch():
    scratch = []
    for count in (16, 8, 4, 3):
        scratch += [pltpu.VMEM((count,) + SHARD[w], kind_of(w)) for w in range(5)]
    return scratch


def scatter_kernel(*refs):
    ins, outs, acc = refs[:5], refs[5:10], refs[10:15]
    slots = [refs[15 + 5 * i : 20 + 5 * i] for i in range(4)]
    send_sem, recv_sem, local_sem = refs[35:]
    s = Reduce(acc, *slots, send_sem, recv_sem)
    loads = [pltpu.make_async_copy(ins[w], acc[w], local_sem.at[w]) for w in range(5)]
    waves = (3, 2, 0, 1, 4)
    for w in waves:
        loads[w].start()
    meet(*s.at)
    for i in range(len(waves) + 3):
        if i < len(waves):
            loads[waves[i]].wait()
            s.open(waves[i])
        for stage in range(3):
            j = i - stage
            if 0 <= j < len(waves):
                s.fold(waves[j], stage)
        j = i - 3
        if 0 <= j < len(waves):
            s.finish(waves[j], outs[waves[j]])
    for w in waves:
        s.close(w)


def scatter_all(*grads):
    return pl.pallas_call(
        scatter_kernel,
        out_shape=[jax.ShapeDtypeStruct(shape, jnp.float32) for shape in SHARD],
        in_specs=[pl.BlockSpec(memory_space=pl.ANY)] * 5,
        out_specs=[pl.BlockSpec(memory_space=pltpu.VMEM)] * 5,
        scratch_shapes=[pltpu.VMEM(GATHERED[w], kind_of(w)) for w in range(5)]
        + reduce_scratch()
        + [
            pltpu.SemaphoreType.DMA((5, 31)),
            pltpu.SemaphoreType.DMA((5, 31)),
            pltpu.SemaphoreType.DMA((5,)),
        ],
        compiler_params=pltpu.CompilerParams(
            collective_id=1, has_side_effects=True, vmem_limit_bytes=60 * 1024 * 1024
        ),
        name="scatter_grads",
    )(*grads)


def fits(mesh):
    return dict(mesh.shape) == {"rows": NZ * NX, "head": NY * NC}


def shards(*args, fast):
    return shards_fast(*args) if fast else shards_plain(*args)


def shards_fast(
    inputs,
    qkv_weight,
    out_weight,
    up_weight,
    down_weight,
    biases,
    norm_params,
    cotangent,
    boundaries,
    lengths,
):
    micro, seq_per, seq, width = inputs.shape
    count = micro * seq_per
    heads = width // HD
    groups = NY * NC
    small = jnp.concatenate([biases, norm_params], axis=0).astype(jnp.float32)
    small = jnp.pad(small, ((0, 5), (0, 32)))
    qkv_full, out_full, up_full, down_t, small_full = gather_all(
        qkv_weight, out_weight, up_weight, down_weight.T, small
    )
    qkv_full = qkv_full.reshape(groups, width, -1)
    out_full = out_full.reshape(groups, width, -1)
    bias_float = small_full[:, :, :2, :96].transpose(0, 2, 1, 3).reshape(8, width)
    norm_float = small_full[:, :, 2, :96].reshape(4, width)
    first_seq = lax.axis_index("head") * seq_per
    bounds = lax.dynamic_slice_in_dim(boundaries, first_seq, seq_per, 1).reshape(count)
    lens = lax.dynamic_slice_in_dim(lengths, first_seq, seq_per, 1).reshape(count)

    tokens = inputs.reshape(count * seq, width)
    zero_part = jnp.zeros((heads, HD), jnp.float32)
    head_bias = jnp.stack(
        [bias_float[0].reshape(heads, HD), zero_part, bias_float[1].reshape(heads, HD)], axis=1
    ).reshape(3 * width)
    project = jnp.einsum("td,gde->tge", tokens, qkv_full, preferred_element_type=jnp.float32)
    project = (project.reshape(-1, 3 * width) + head_bias).astype(jnp.bfloat16)
    items = project.reshape(count, seq, heads, 3, HD)
    q, k, v = items[:, :, :, 0], items[:, :, :, 1], items[:, :, :, 2]
    context, log_total = jax.vmap(attend_forward)(q, k, v, bounds, lens)
    context = context.reshape(count * seq, width)
    attended = jnp.einsum("td,gde->tge", context, out_full, preferred_element_type=jnp.float32)
    attended = attended.reshape(-1, width) + bias_float[2]
    hidden, normed_one, scale_one = norm_forward(
        tokens.astype(jnp.float32) + attended, norm_float[0], norm_float[1]
    )
    hidden_low = hidden.astype(jnp.bfloat16)
    inner_pre = jnp.dot(hidden_low, up_full, preferred_element_type=jnp.float32) + bias_float[
        4:8
    ].reshape(-1)
    cdf = 0.5 * (1.0 + lax.erf(inner_pre * ROOT_HALF))
    active_low = (inner_pre * cdf).astype(jnp.bfloat16)
    slope = cdf + inner_pre * jnp.exp(-0.5 * inner_pre * inner_pre) * INVERSE_ROOT_TWO_PI
    outer_out = contract_cols(active_low, down_t) + bias_float[3]
    output_float, normed_two, scale_two = norm_forward(
        hidden + outer_out, norm_float[2], norm_float[3]
    )
    grad_out = cotangent.reshape(count * seq, width).astype(jnp.float32)
    grad_two, gain_two, shift_two = norm_backward(grad_out, normed_two, scale_two, norm_float[2])
    grad_two_low = grad_two.astype(jnp.bfloat16)
    down_grad = contract_rows(grad_two_low, active_low).astype(jnp.bfloat16)
    grad_inner = jnp.dot(grad_two_low, down_t, preferred_element_type=jnp.float32) * slope
    grad_inner_low = grad_inner.astype(jnp.bfloat16)
    up_grad = contract_rows(hidden_low, grad_inner_low).astype(jnp.bfloat16)
    grad_hidden = contract_cols(grad_inner_low, up_full) + grad_two
    grad_one, gain_one, shift_one = norm_backward(grad_hidden, normed_one, scale_one, norm_float[0])
    grad_one_low = grad_one.astype(jnp.bfloat16)
    grad_one_parts = grad_one_low.reshape(-1, groups, width // groups)
    out_grad = jnp.einsum(
        "td,tge->gde", context, grad_one_parts, preferred_element_type=jnp.float32
    ).astype(jnp.bfloat16).reshape(GATHERED[1])
    grad_context = jnp.einsum(
        "tge,gde->td", grad_one_parts, out_full, preferred_element_type=jnp.float32
    ).astype(jnp.bfloat16)
    grad_items = grad_context.reshape(count, seq, heads, HD)
    grad_project = jax.vmap(attend_backward)(q, k, v, bounds, lens, log_total, grad_items)
    grad_project = grad_project.reshape(count * seq, 3 * width)
    parts = grad_project.reshape(count * seq, groups, -1)
    qkv_grad = jnp.einsum(
        "td,tge->gde", tokens, parts, preferred_element_type=jnp.float32
    ).astype(jnp.bfloat16).reshape(GATHERED[0])
    grad_input = (
        jnp.einsum("tge,gde->td", parts, qkv_full, preferred_element_type=jnp.float32) + grad_one
    )
    project_sums = jnp.sum(grad_project, axis=0, dtype=jnp.float32).reshape(heads, 3, HD)
    bias_grad = jnp.concatenate(
        [
            project_sums[:, 0].reshape(1, width),
            project_sums[:, 2].reshape(1, width),
            jnp.sum(grad_one, axis=0).reshape(1, width),
            jnp.sum(grad_two, axis=0).reshape(1, width),
            jnp.sum(grad_inner, axis=0).reshape(4, width),
        ],
        axis=0,
    )
    norm_grad = jnp.stack([gain_one, shift_one, gain_two, shift_two])
    small_grad = jnp.concatenate(
        [
            bias_grad.reshape(groups, 2, 8, 96).transpose(0, 2, 1, 3),
            norm_grad.reshape(groups, 1, 8, 96).transpose(0, 2, 1, 3),
        ],
        axis=2,
    )
    small_grad = jnp.pad(small_grad, ((0, 0), (0, 0), (0, 5), (0, 32)))
    own = scatter_all(qkv_grad, out_grad, up_grad, down_grad, small_grad)
    return (
        output_float.astype(jnp.bfloat16).reshape(inputs.shape),
        grad_input.reshape(inputs.shape),
        own[0],
        own[1],
        own[2],
        own[3].T,
        own[4][:2, :96],
        own[4][2:3, :96],
    )


def solution(mesh):
    tokens = P(None, ("rows", "head"), None, None)
    weight = P("rows", "head")
    small = P("head", "rows")
    per_row = P(None, "rows")
    return jax.shard_map(
        functools.partial(shards, fast=fits(mesh)),
        mesh=mesh,
        in_specs=(tokens, weight, weight, weight, weight, small, small, tokens, per_row, per_row),
        out_specs=(tokens, tokens, weight, weight, weight, weight, small, small),
        check_vma=False,
    )
```

```python
import functools

import jax
import jax.numpy as jnp
from jax import lax
from jax.experimental import pallas as pl
from jax.experimental.pallas import tpu as pltpu
from jax.sharding import PartitionSpec as P

HD = 64
EPSILON = 1e-06
ROOT_HALF = 0.7071067811865476
INVERSE_ROOT_TWO_PI = 0.3989422804014327
AXES = ("rows", "head")


def contract_rows(left, right):
    return lax.dot_general(
        left, right, (((0,), (0,)), ((), ())), preferred_element_type=jnp.float32
    )


def contract_cols(left, right):
    return lax.dot_general(
        left, right, (((1,), (1,)), ((), ())), preferred_element_type=jnp.float32
    )


def norm_forward(values_in, gain_row, shift_row):
    average = jnp.mean(values_in, axis=-1, keepdims=True)
    centered = values_in - average
    variance = jnp.mean(centered * centered, axis=-1, keepdims=True)
    inverse_scale = lax.rsqrt(variance + EPSILON)
    normed = centered * inverse_scale
    return (normed * gain_row + shift_row, normed, inverse_scale)


def norm_backward(grad_out, normed, inverse_scale, gain_row):
    grad_normed = grad_out * gain_row
    first_mean = jnp.mean(grad_normed, axis=-1, keepdims=True)
    second_mean = jnp.mean(grad_normed * normed, axis=-1, keepdims=True)
    grad_in = inverse_scale * (grad_normed - first_mean - normed * second_mean)
    return (grad_in, jnp.sum(grad_out * normed, axis=0), jnp.sum(grad_out, axis=0))


def masked_scores(queries, keys_in, bound, length):
    seq = queries.shape[0]
    positions = lax.broadcasted_iota(jnp.int32, (seq,), 0)
    segment = positions >= bound
    allowed = (segment[:, None] == segment[None, :]) & (positions[None, :] < length)
    scores = jnp.einsum(
        "qhe,khe->hqk", queries, keys_in, preferred_element_type=jnp.float32
    ) * HD ** (-0.5)
    return jnp.where(allowed[None], scores, -1e30)


def attend_forward(queries, keys_in, values_in, bound, length):
    scores = masked_scores(queries, keys_in, bound, length)
    highest = jnp.max(scores, axis=-1, keepdims=True)
    raised = jnp.exp(scores - highest)
    totals = jnp.sum(raised, axis=-1, keepdims=True)
    weights_low = (raised / totals).astype(jnp.bfloat16)
    context = jnp.einsum("hqk,khe->qhe", weights_low, values_in, preferred_element_type=jnp.float32)
    log_total = (highest + jnp.log(totals))[..., 0]
    return (context.astype(jnp.bfloat16), log_total)


def attend_backward(queries, keys_in, values_in, bound, length, log_total, grad_context):
    scores = masked_scores(queries, keys_in, bound, length)
    weights_full = jnp.exp(scores - log_total[..., None])
    weights_low = weights_full.astype(jnp.bfloat16)
    grad_values = jnp.einsum(
        "hqk,qhe->khe", weights_low, grad_context, preferred_element_type=jnp.float32
    )
    grad_weights = jnp.einsum(
        "qhe,khe->hqk", grad_context, values_in, preferred_element_type=jnp.float32
    )
    inner_sum = jnp.sum(weights_full * grad_weights, axis=-1, keepdims=True)
    grad_scores = (weights_full * (grad_weights - inner_sum)).astype(jnp.bfloat16)
    grad_queries = jnp.einsum(
        "hqk,khe->qhe", grad_scores, keys_in, preferred_element_type=jnp.float32
    ) * HD ** (-0.5)
    grad_keys = jnp.einsum(
        "hqk,qhe->khe", grad_scores, queries, preferred_element_type=jnp.float32
    ) * HD ** (-0.5)
    return jnp.stack([grad_queries, grad_keys, grad_values], axis=2).astype(jnp.bfloat16)


def gather(shard, row_axis):
    rows, head = lax.axis_size("rows"), lax.axis_size("head")
    a, b = shard.shape
    every = lax.all_gather(shard, AXES, axis=0, tiled=False).reshape(rows, head, a, b)
    if row_axis == 0:
        return every.transpose(0, 2, 1, 3).reshape(rows * a, head * b)
    return every.transpose(1, 2, 0, 3).reshape(head * a, rows * b)


def scatter(grad, row_axis):
    rows, head = lax.axis_size("rows"), lax.axis_size("head")
    a, b = grad.shape
    if row_axis == 0:
        parts = grad.reshape(rows, a // rows, head, b // head).transpose(0, 2, 1, 3)
    else:
        parts = grad.reshape(head, a // head, rows, b // rows).transpose(2, 0, 1, 3)
    parts = parts.reshape((rows * head,) + parts.shape[2:]).astype(jnp.bfloat16)
    return lax.psum_scatter(parts, AXES, scatter_dimension=0, tiled=False).astype(jnp.float32)


def shards_plain(
    inputs,
    qkv_weight,
    out_weight,
    up_weight,
    down_weight,
    biases,
    norm_params,
    cotangent,
    boundaries,
    lengths,
):
    micro, seq_per, seq, width = inputs.shape
    count = micro * seq_per
    heads = width // HD
    qkv_full, out_full, up_full, down_full = (
        gather(w, 0) for w in (qkv_weight, out_weight, up_weight, down_weight)
    )
    bias_float = gather(biases, 1).astype(jnp.float32)
    norm_float = gather(norm_params, 1).astype(jnp.float32)
    first_seq = lax.axis_index("head") * seq_per
    bounds = lax.dynamic_slice_in_dim(boundaries, first_seq, seq_per, 1).reshape(count)
    lens = lax.dynamic_slice_in_dim(lengths, first_seq, seq_per, 1).reshape(count)

    tokens = inputs.reshape(count * seq, width)
    zero_part = jnp.zeros((heads, HD), jnp.float32)
    head_bias = jnp.stack(
        [bias_float[0].reshape(heads, HD), zero_part, bias_float[1].reshape(heads, HD)], axis=1
    ).reshape(3 * width)
    project = (jnp.dot(tokens, qkv_full, preferred_element_type=jnp.float32) + head_bias).astype(
        jnp.bfloat16
    )
    items = project.reshape(count, seq, heads, 3, HD)
    q, k, v = items[:, :, :, 0], items[:, :, :, 1], items[:, :, :, 2]
    context, log_total = jax.vmap(attend_forward)(q, k, v, bounds, lens)
    context = context.reshape(count * seq, width)
    attended = jnp.dot(context, out_full, preferred_element_type=jnp.float32) + bias_float[2]
    hidden, normed_one, scale_one = norm_forward(
        tokens.astype(jnp.float32) + attended, norm_float[0], norm_float[1]
    )
    hidden_low = hidden.astype(jnp.bfloat16)
    inner_pre = jnp.dot(hidden_low, up_full, preferred_element_type=jnp.float32) + bias_float[
        4:8
    ].reshape(-1)
    cdf = 0.5 * (1.0 + lax.erf(inner_pre * ROOT_HALF))
    active_low = (inner_pre * cdf).astype(jnp.bfloat16)
    slope = cdf + inner_pre * jnp.exp(-0.5 * inner_pre * inner_pre) * INVERSE_ROOT_TWO_PI
    outer_out = jnp.dot(active_low, down_full, preferred_element_type=jnp.float32) + bias_float[3]
    output_float, normed_two, scale_two = norm_forward(
        hidden + outer_out, norm_float[2], norm_float[3]
    )
    grad_out = cotangent.reshape(count * seq, width).astype(jnp.float32)
    grad_two, gain_two, shift_two = norm_backward(grad_out, normed_two, scale_two, norm_float[2])
    grad_two_low = grad_two.astype(jnp.bfloat16)
    down_grad = scatter(contract_rows(active_low, grad_two_low), 0)
    grad_inner = contract_cols(grad_two_low, down_full) * slope
    grad_inner_low = grad_inner.astype(jnp.bfloat16)
    up_grad = scatter(contract_rows(hidden_low, grad_inner_low), 0)
    grad_hidden = contract_cols(grad_inner_low, up_full) + grad_two
    grad_one, gain_one, shift_one = norm_backward(grad_hidden, normed_one, scale_one, norm_float[0])
    grad_one_low = grad_one.astype(jnp.bfloat16)
    out_grad = scatter(contract_rows(context, grad_one_low), 0)
    grad_context = contract_cols(grad_one_low, out_full).astype(jnp.bfloat16)
    grad_items = grad_context.reshape(count, seq, heads, HD)
    grad_project = jax.vmap(attend_backward)(q, k, v, bounds, lens, log_total, grad_items)
    grad_project = grad_project.reshape(count * seq, 3 * width)
    qkv_grad = scatter(contract_rows(tokens, grad_project), 0)
    grad_input = contract_cols(grad_project, qkv_full) + grad_one
    project_sums = jnp.sum(grad_project, axis=0, dtype=jnp.float32).reshape(heads, 3, HD)
    bias_grad = jnp.concatenate(
        [
            project_sums[:, 0].reshape(1, width),
            project_sums[:, 2].reshape(1, width),
            jnp.sum(grad_one, axis=0).reshape(1, width),
            jnp.sum(grad_two, axis=0).reshape(1, width),
            jnp.sum(grad_inner, axis=0).reshape(4, width),
        ],
        axis=0,
    )
    norm_grad = jnp.stack([gain_one, shift_one, gain_two, shift_two])
    return (
        output_float.astype(jnp.bfloat16).reshape(inputs.shape),
        grad_input.reshape(inputs.shape),
        qkv_grad,
        out_grad,
        up_grad,
        down_grad,
        scatter(bias_grad, 1),
        scatter(norm_grad, 1),
    )


MESH = pl.DeviceIdType.MESH
NZ, NX, NY, NC = 4, 2, 2, 2
FIRST = ("x", "x", "y", "y", "x")


def spot():
    r, h = lax.axis_index("rows"), lax.axis_index("head")
    return r // NX, lax.rem(r, NX), h // NC, lax.rem(h, NC)


def dev(z, x, y, c):
    return (z * NX + x, y * NC + c)


def other_z(z, d):
    return lax.rem(z + d, NZ)


def meet(z, x, y, c):
    barrier = pltpu.get_barrier_semaphore()
    mates = [dev(other_z(z, d), x, y, c) for d in range(1, NZ)]
    mates += [dev(z, 1 - x, y, c), dev(z, x, 1 - y, c), dev(z, x, y, 1 - c)]
    for mate in mates:
        pl.semaphore_signal(barrier, inc=1, device_id=mate, device_id_type=MESH)
    pl.semaphore_wait(barrier, len(mates))


def tile(w, ref, z, x, y, c):
    r, h = dev(z, x, y, c)
    if w == 2:
        return ref.at[pl.ds(pl.multiple_of(r * 96, 32), 96), pl.ds(pl.multiple_of(h * 768, 128), 768)]
    if w == 3:
        return ref.at[pl.ds(pl.multiple_of(h * 192, 64), 192), pl.ds(pl.multiple_of(r * 384, 128), 384)]
    return ref.at[h, r]


class Spread:
    def __init__(self, ins, outs, send_sem, recv_sem, local_sem):
        self.ins, self.outs = ins, outs
        self.send_sem, self.recv_sem, self.local_sem = send_sem, recv_sem, local_sem
        self.at = spot()
        self.sent = {w: [] for w in range(5)}
        self.locals = {}

    def push(self, w, src, shard, to):
        k = len(self.sent[w])
        copy = pltpu.make_async_remote_copy(
            src_ref=src,
            dst_ref=tile(w, self.outs[w], *shard),
            send_sem=self.send_sem.at[w, k],
            recv_sem=self.recv_sem.at[w, self.index(shard)],
            device_id=to,
            device_id_type=MESH,
        )
        copy.start()
        self.sent[w].append(copy)

    def index(self, shard):
        r, h = dev(*shard)
        return r * (NY * NC) + h

    def take(self, w, shard):
        there = tile(w, self.outs[w], *shard)
        pltpu.make_async_remote_copy(
            src_ref=there,
            dst_ref=there,
            send_sem=self.send_sem.at[w, 0],
            recv_sem=self.recv_sem.at[w, self.index(shard)],
            device_id=dev(self.at[0], self.at[1], self.at[2], 1 - self.at[3]),
            device_id_type=MESH,
        ).wait_recv()

    def spread(self, w, src, shard, kinds):
        z, x, y, c = self.at
        to = {"x": dev(z, 1 - x, y, c), "y": dev(z, x, 1 - y, c), "c": dev(z, x, y, 1 - c)}
        for kind in kinds:
            self.push(w, src, shard, to[kind])

    def open(self, w):
        z, x, y, c = self.at
        src = self.ins[w]
        for d in range(1, NZ):
            self.push(w, src, self.at, dev(other_z(z, d), x, y, c))
        second = "y" if FIRST[w] == "x" else "x"
        self.spread(w, src, self.at, (FIRST[w], second, "c"))
        local = pltpu.make_async_copy(src, tile(w, self.outs[w], *self.at), self.local_sem.at[w])
        local.start()
        self.locals[w] = local

    def near(self, w):
        z, x, y, c = self.at
        second = "y" if FIRST[w] == "x" else "x"
        for d in range(1, NZ):
            shard = (other_z(z, d), x, y, c)
            self.take(w, shard)
            self.spread(w, tile(w, self.outs[w], *shard), shard, (FIRST[w], second, "c"))

    def middle(self, w):
        z, x, y, c = self.at
        second = "y" if FIRST[w] == "x" else "x"
        for d in range(NZ):
            shard = (other_z(z, d), 1 - x, y, c) if FIRST[w] == "x" else (other_z(z, d), x, 1 - y, c)
            self.take(w, shard)
            self.spread(w, tile(w, self.outs[w], *shard), shard, (second, "c"))

    def far(self, w):
        z, x, y, c = self.at
        for e in range(2):
            for d in range(NZ):
                if FIRST[w] == "x":
                    shard = (other_z(z, d), x if e == 0 else 1 - x, 1 - y, c)
                else:
                    shard = (other_z(z, d), 1 - x, y if e == 0 else 1 - y, c)
                self.take(w, shard)
                self.spread(w, tile(w, self.outs[w], *shard), shard, ("c",))

    def core(self, w):
        z, x, y, c = self.at
        for ey in range(2):
            for ex in range(2):
                for d in range(NZ):
                    self.take(
                        w,
                        (other_z(z, d), x if ex == 0 else 1 - x, y if ey == 0 else 1 - y, 1 - c),
                    )

    def settle(self, w):
        self.locals.pop(w).wait()

    def close(self):
        for local in self.locals.values():
            local.wait()
        for copies in self.sent.values():
            for copy in copies:
                copy.wait_send()


def gather_kernel(*refs):
    ins, outs = refs[:5], refs[5:10]
    s = Spread(ins, outs, *refs[10:])
    meet(*s.at)
    s.open(0)
    s.open(4)
    s.near(0)
    for w in (1, 2, 3):
        s.open(w)
    s.near(4)
    s.middle(0)
    s.near(1)
    s.middle(4)
    s.near(2)
    s.far(0)
    s.far(4)
    s.middle(1)
    s.near(3)
    s.middle(2)
    s.far(1)
    s.middle(3)
    s.far(2)
    s.far(3)
    for w in range(5):
        s.core(w)
    s.close()


GATHERED = ((4, 8, 96, 576), (4, 8, 96, 192), (768, 3072), (768, 3072), (4, 8, 8, 128))


def gather_all(qkv, out, up, down_t, small):
    return pl.pallas_call(
        gather_kernel,
        out_shape=[
            jax.ShapeDtypeStruct(shape, jnp.float32 if i == 4 else jnp.bfloat16)
            for i, shape in enumerate(GATHERED)
        ],
        in_specs=[pl.BlockSpec(memory_space=pltpu.VMEM)] * 5,
        out_specs=[pl.BlockSpec(memory_space=pl.ANY)] * 5,
        scratch_shapes=[
            pltpu.SemaphoreType.DMA((5, 31)),
            pltpu.SemaphoreType.DMA((5, 32)),
            pltpu.SemaphoreType.DMA((5,)),
        ],
        compiler_params=pltpu.CompilerParams(collective_id=0, has_side_effects=True),
        name="gather_weights",
    )(qkv, out, up, down_t, small)


SHARD = ((96, 576), (96, 192), (96, 768), (192, 384), (8, 128))


def kind_of(w):
    return jnp.float32 if w == 4 else jnp.bfloat16


class Reduce:
    def __init__(self, acc, from_core, from_second, from_first, from_z, send_sem, recv_sem):
        self.acc = acc
        self.slots = (from_core, from_second, from_first, from_z)
        self.send_sem, self.recv_sem = send_sem, recv_sem
        self.at = spot()

    def shard(self, w, d, e1, e2, ec):
        z, x, y, c = self.at
        flip = lambda v, e: v + e * (1 - 2 * v)
        ex, ey = (e1, e2) if FIRST[w] == "x" else (e2, e1)
        return (other_z(z, d), flip(x, ex), flip(y, ey), flip(c, ec))

    def order(self, stage, k):
        if stage == 0:
            return (lax.rem(k, 4), 1 - lax.rem(k // 4, 2), 1 - k // 8)
        if stage == 1:
            return (lax.rem(k, 4), 1 - k // 4, 0)
        return (lax.rem(k + 1, 4), 0, 0)

    def slot(self, w, stage, shard):
        z, x, y, c = shard
        first, second = (x, y) if FIRST[w] == "x" else (y, x)
        if stage == 0:
            return (z * 2 + first) * 2 + second
        if stage == 1:
            return z * 2 + first
        return z

    def sending(self, w, stage, k):
        z, x, y, c = self.at
        if stage == 0:
            shard = self.shard(w, lax.rem(k, 4), 1 - lax.rem(k // 4, 2), 1 - k // 8, 1)
            to, place, base = dev(z, x, y, 1 - c), self.slot(w, 0, shard), 0
        elif stage == 1:
            shard = self.shard(w, lax.rem(k, 4), 1 - k // 4, 1, 0)
            to = dev(z, x, 1 - y, c) if FIRST[w] == "x" else dev(z, 1 - x, y, c)
            place, base = self.slot(w, 1, shard), 16
        elif stage == 2:
            shard = self.shard(w, lax.rem(k + 1, 4), 1, 0, 0)
            to = dev(z, 1 - x, y, c) if FIRST[w] == "x" else dev(z, x, 1 - y, c)
            place, base = self.slot(w, 2, shard), 24
        else:
            shard = self.shard(w, k + 1, 0, 0, 0)
            to, place, base = dev(other_z(z, k + 1), x, y, c), k, 28
        return pltpu.make_async_remote_copy(
            src_ref=tile(w, self.acc[w], *shard),
            dst_ref=self.slots[stage][w].at[place],
            send_sem=self.send_sem.at[w, base + k],
            recv_sem=self.recv_sem.at[w, base + place],
            device_id=to,
            device_id_type=MESH,
        )

    def arrive(self, w, stage, place):
        z, x, y, c = self.at
        here = self.slots[stage][w].at[place]
        base = (0, 16, 24, 28)[stage]
        pltpu.make_async_remote_copy(
            src_ref=here,
            dst_ref=here,
            send_sem=self.send_sem.at[w, base],
            recv_sem=self.recv_sem.at[w, base + place],
            device_id=dev(z, x, y, 1 - c),
            device_id_type=MESH,
        ).wait_recv()

    def open(self, w):
        def step(k, carry):
            self.sending(w, 0, k).start()
            return carry

        lax.fori_loop(0, 16, step, 0)

    def fold(self, w, stage):
        count = (16, 8, 4)[stage]
        leave = (8, 4, 3)[stage]

        def step(k, carry):
            d, e1, e2 = self.order(stage, k)
            shard = self.shard(w, d, e1, e2, 0)
            place = self.slot(w, stage, shard)
            self.arrive(w, stage, place)
            mine = tile(w, self.acc[w], *shard)
            total = mine[...].astype(jnp.float32) + self.slots[stage][w][place].astype(jnp.float32)
            mine[...] = total.astype(kind_of(w))

            @pl.when(jnp.logical_and(k >= 1, k <= leave))
            def _():
                self.sending(w, stage + 1, k - 1).start()

            return carry

        lax.fori_loop(0, count, step, 0)

    def finish(self, w, out):
        total = tile(w, self.acc[w], *self.at)[...].astype(jnp.float32)
        for k in range(3):
            self.arrive(w, 3, k)
            total = total + self.slots[3][w][k].astype(jnp.float32)
        out[...] = total

    def close(self, w):
        for stage, count in enumerate((16, 8, 4, 3)):

            def step(k, carry, stage=stage):
                self.sending(w, stage, k).wait_send()
                return carry

            lax.fori_loop(0, count, step, 0)


def reduce_scratch():
    scratch = []
    for count in (16, 8, 4, 3):
        scratch += [pltpu.VMEM((count,) + SHARD[w], kind_of(w)) for w in range(5)]
    return scratch


def scatter_kernel(*refs):
    ins, outs, acc = refs[:5], refs[5:10], refs[10:15]
    slots = [refs[15 + 5 * i : 20 + 5 * i] for i in range(4)]
    send_sem, recv_sem, local_sem = refs[35:]
    s = Reduce(acc, *slots, send_sem, recv_sem)
    loads = [pltpu.make_async_copy(ins[w], acc[w], local_sem.at[w]) for w in range(5)]
    waves = (3, 2, 0, 1, 4)
    for w in waves:
        loads[w].start()
    meet(*s.at)
    for i in range(len(waves) + 3):
        if i < len(waves):
            loads[waves[i]].wait()
            s.open(waves[i])
        for stage in range(3):
            j = i - stage
            if 0 <= j < len(waves):
                s.fold(waves[j], stage)
        j = i - 3
        if 0 <= j < len(waves):
            s.finish(waves[j], outs[waves[j]])
    for w in waves:
        s.close(w)


def scatter_all(*grads):
    return pl.pallas_call(
        scatter_kernel,
        out_shape=[jax.ShapeDtypeStruct(shape, jnp.float32) for shape in SHARD],
        in_specs=[pl.BlockSpec(memory_space=pl.ANY)] * 5,
        out_specs=[pl.BlockSpec(memory_space=pltpu.VMEM)] * 5,
        scratch_shapes=[pltpu.VMEM(GATHERED[w], kind_of(w)) for w in range(5)]
        + reduce_scratch()
        + [
            pltpu.SemaphoreType.DMA((5, 31)),
            pltpu.SemaphoreType.DMA((5, 31)),
            pltpu.SemaphoreType.DMA((5,)),
        ],
        compiler_params=pltpu.CompilerParams(
            collective_id=1, has_side_effects=True, vmem_limit_bytes=60 * 1024 * 1024
        ),
        name="scatter_grads",
    )(*grads)


F32, BF16 = jnp.float32, jnp.bfloat16


def fits(mesh):
    return dict(mesh.shape) == {"rows": NZ * NX, "head": NY * NC}


def shards(*args, fast):
    return shards_fast(*args) if fast else shards_plain(*args)


def mul(left, right, left_dim, right_dim):
    return lax.dot_general(
        left, right, (((left_dim,), (right_dim,)), ((), ())), preferred_element_type=F32
    )


def fill_mask(mask, bounds, lens, column):
    seq = mask.shape[1]
    key = lax.broadcasted_iota(jnp.int32, (seq, seq), 0)
    query = lax.broadcasted_iota(jnp.int32, (seq, seq), 1)
    for m in range(mask.shape[0]):
        bound, length = bounds[m, column], lens[m, column]
        same = (key >= bound) == (query >= bound)
        mask[m] = jnp.where(jnp.logical_and(same, key < length), 0.0, -1e30).astype(F32)


def group_of(k, y, c):
    return (y if k < 2 else 1 - y) * NC + (c if k % 2 == 0 else 1 - c)


def project_group(g, weight, x_t, bias_t, project):
    w = weight[g].reshape(x_t.shape[0], project.shape[1])
    first = pl.multiple_of(g * 192, 64)
    for m in range(2):
        cols = pl.ds(m * 512, 512)
        full = mul(w, x_t[:, cols], 0, 0)
        for j in range(3):
            rows = pl.ds(first + 64 * j, 64)
            a = 192 * j
            q = (full[a : a + 64] + bias_t[rows, 0:1]).astype(BF16)
            project[g, a : a + 64, cols] = q * jnp.asarray(0.125, BF16)
            project[g, a + 64 : a + 128, cols] = full[a + 64 : a + 128].astype(BF16)
            v = full[a + 128 : a + 192] + bias_t[rows, 1:2]
            project[g, a + 128 : a + 192, cols] = v.astype(BF16)


def attend_group(g, m, project, mask, context, log_total):
    def head(j, carry):
        base = pl.multiple_of(j * 192, 64)
        cols = pl.ds(m * 512, 512)
        keys = project[g, pl.ds(base + 64, 64), cols]
        values = project[g, pl.ds(base + 128, 64), cols]
        for part in range(2):
            some = pl.ds(m * 512 + part * 256, 256)
            queries = project[g, pl.ds(base, 64), some]
            s = mul(keys, queries, 0, 0) + mask[m, :, part * 256 : part * 256 + 256]
            highest = jnp.max(s, axis=0, keepdims=True)
            p = jnp.exp(s - highest)
            total = jnp.sum(p, axis=0, keepdims=True)
            low = (p * (1.0 / total)).astype(BF16)
            context[g, pl.ds(pl.multiple_of(j * 64, 64), 64), some] = mul(
                values, low, 1, 0
            ).astype(BF16)
            log_total[g, m * 3 + j, :, part * 256 : part * 256 + 256] = highest + jnp.log(total)
        return carry

    lax.fori_loop(0, 3, head, 0)


def attend_group_back(g, m, project, mask, log_total, grad_context, grads):
    def head(j, carry):
        base = pl.multiple_of(j * 192, 64)
        cols = pl.ds(m * 512, 512)
        keys = project[g, pl.ds(base + 64, 64), cols]
        values = project[g, pl.ds(base + 128, 64), cols]
        grad_k = jnp.zeros((64, 512), F32)
        grad_v = jnp.zeros((64, 512), F32)
        for part in range(2):
            some = pl.ds(m * 512 + part * 256, 256)
            queries = project[g, pl.ds(base, 64), some]
            grad_out = grad_context[g, pl.ds(pl.multiple_of(j * 64, 64), 64), some]
            s = mul(keys, queries, 0, 0) + mask[m, :, part * 256 : part * 256 + 256]
            p = jnp.exp(s - log_total[g, m * 3 + j, :, part * 256 : part * 256 + 256])
            grad_v = grad_v + mul(grad_out, p.astype(BF16), 1, 1)
            grad_p = mul(values, grad_out, 0, 0)
            inner = jnp.sum(p * grad_p, axis=0, keepdims=True)
            grad_s = (p * (grad_p - inner)).astype(BF16)
            grads[pl.ds(base, 64), some] = (mul(keys, grad_s, 1, 0) * 0.125).astype(BF16)
            grad_k = grad_k + mul(queries, grad_s, 1, 1)
        grads[pl.ds(base + 64, 64), cols] = grad_k.astype(BF16)
        grads[pl.ds(base + 128, 64), cols] = grad_v.astype(BF16)
        return carry

    lax.fori_loop(0, 3, head, 0)


def join_small(small, rows_out, cols_out):
    width = rows_out.shape[1]
    total = jnp.zeros(rows_out.shape, F32)
    for r in range(NZ * NX):
        part = small[:, r].reshape(32, 128).astype(BF16)
        i = lax.broadcasted_iota(jnp.int32, (128, width), 0)
        j = lax.broadcasted_iota(jnp.int32, (128, width), 1)
        place = jnp.logical_and(j == i + 96 * r, i < 96)
        total = total + mul(part, jnp.where(place, 1.0, 0.0).astype(BF16), 1, 0)
    rows_out[...] = total
    eye = lax.broadcasted_iota(jnp.int32, (width, width), 0) == lax.broadcasted_iota(
        jnp.int32, (width, width), 1
    )
    cols_out[...] = mul(jnp.where(eye, 1.0, 0.0).astype(BF16), total.astype(BF16), 1, 1)


def row(rows, b):
    at = 8 * (b // 2) + b % 2 if b < 8 else 8 * (b - 8) + 2
    return rows[at : at + 1, :]


def normalize(z):
    centered = z - jnp.mean(z, axis=-1, keepdims=True)
    scale = lax.rsqrt(jnp.mean(centered * centered, axis=-1, keepdims=True) + EPSILON)
    return centered * scale, scale


def forward_kernel(*refs):
    ins, x, bounds, lens = refs[:5], refs[5], refs[6], refs[7]
    (qkv_o, out_o, up_o, down_o, rows_o, project_o, total_o, context_o, normed_o, scale_o,
     hidden_o, active_o, slope_o) = refs[8:21]
    (qkv, out, up, small, x_t, cols, mask, project, context, out_cat, active, slope,
     send_sem, recv_sem, local_sem, copy_sem) = refs[21:]
    s = Spread(ins, (qkv, out, up, down_o, small), send_sem, recv_sem, local_sem)
    z_at, x_at, y, c = s.at
    meet(*s.at)
    s.open(0)
    s.open(4)
    x_t[...] = x[...].T
    s.near(0)
    s.near(4)
    s.middle(0)
    s.middle(4)
    for w in (1, 2, 3):
        s.open(w)
    fill_mask(mask, bounds, lens, lax.axis_index("head"))
    s.far(4)
    s.core(4)
    s.settle(4)
    join_small(small, rows_o, cols)
    s.settle(0)

    def unit(k, m):
        attend_group(group_of(k, y, c), m, project, mask, context, total_o)

    def proj(k):
        project_group(group_of(k, y, c), qkv, x_t, cols, project)

    proj(0)
    s.near(1)
    s.near(2)
    unit(0, 0)
    s.far(0)
    s.near(3)
    unit(0, 1)
    s.middle(1)
    s.core(0)
    s.middle(2)
    proj(1)
    unit(1, 0)
    s.far(1)
    s.middle(3)
    unit(1, 1)
    s.core(1)
    s.settle(1)
    proj(2)
    unit(2, 0)
    s.far(2)
    proj(3)
    unit(2, 1)
    copies = [
        pltpu.make_async_copy(qkv, qkv_o, copy_sem.at[0]),
        pltpu.make_async_copy(project, project_o, copy_sem.at[1]),
    ]
    for copy in copies:
        copy.start()
    unit(3, 0)
    s.far(3)
    unit(3, 1)
    for g in range(4):
        out_cat[:, 192 * g : 192 * g + 192] = out[g].reshape(768, 192)
    more = [
        pltpu.make_async_copy(out_cat, out_o, copy_sem.at[2]),
        pltpu.make_async_copy(context, context_o, copy_sem.at[3]),
    ]
    s.core(2)
    s.settle(2)
    more.append(pltpu.make_async_copy(up, up_o, copy_sem.at[4]))
    for copy in more:
        copy.start()
    copies += more

    def block(b, carry):
        rows = pl.ds(pl.multiple_of(b * 256, 256), 256)
        ctx = context[:, :, rows].reshape(768, 256)
        attended = mul(ctx, out_cat[...], 0, 0) + row(rows_o, 2)
        normed, scale = normalize(x[rows, :].astype(F32) + attended)
        normed_o[rows, :] = normed
        scale_o[rows, :] = jnp.broadcast_to(scale, (256, 128))
        low = (normed * row(rows_o, 8) + row(rows_o, 9)).astype(BF16)
        hidden_o[rows, :] = low
        for n in range(4):
            wide = slice(768 * n, 768 * n + 768)
            inner = mul(low, up[:, wide], 1, 0) + row(rows_o, 4 + n)
            cdf = 0.5 * (1.0 + lax.erf(inner * ROOT_HALF))
            active[rows, wide] = (inner * cdf).astype(BF16)
            bell = jnp.exp(-0.5 * inner * inner) * INVERSE_ROOT_TWO_PI
            slope[rows, wide] = (cdf + inner * bell).astype(BF16)
        return carry

    lax.fori_loop(0, 4, block, 0)
    last = [
        pltpu.make_async_copy(active, active_o, copy_sem.at[5]),
        pltpu.make_async_copy(slope, slope_o, copy_sem.at[6]),
    ]
    for copy in last:
        copy.start()
    s.core(3)
    s.close()
    for copy in copies + last:
        copy.wait()


def forward(qkv, out, up, down_t, small, x, bounds, lens):
    vmem, hbm = pl.BlockSpec(memory_space=pltpu.VMEM), pl.BlockSpec(memory_space=pl.ANY)
    smem = pl.BlockSpec(memory_space=pltpu.SMEM)
    t, d = x.shape
    shape = jax.ShapeDtypeStruct
    return pl.pallas_call(
        forward_kernel,
        out_shape=[
            shape(GATHERED[0], BF16),
            shape((d, d), BF16),
            shape(GATHERED[2], BF16),
            shape(GATHERED[3], BF16),
            shape((32, d), F32),
            shape((4, 576, t), BF16),
            shape((4, 6, 1, 512), F32),
            shape((4, 192, t), BF16),
            shape((t, d), F32),
            shape((t, 128), F32),
            shape((t, d), BF16),
            shape((t, 3072), BF16),
            shape((t, 3072), BF16),
        ],
        in_specs=[vmem] * 6 + [smem] * 2,
        out_specs=[hbm] * 4 + [vmem, hbm, vmem, hbm] + [vmem] * 3 + [hbm] * 2,
        scratch_shapes=[
            pltpu.VMEM(GATHERED[0], BF16),
            pltpu.VMEM(GATHERED[1], BF16),
            pltpu.VMEM(GATHERED[2], BF16),
            pltpu.VMEM(GATHERED[4], F32),
            pltpu.VMEM((d, t), BF16),
            pltpu.VMEM((d, 32), F32),
            pltpu.VMEM((2, 512, 512), F32),
            pltpu.VMEM((4, 576, t), BF16),
            pltpu.VMEM((4, 192, t), BF16),
            pltpu.VMEM((d, d), BF16),
            pltpu.VMEM((t, 3072), BF16),
            pltpu.VMEM((t, 3072), BF16),
            pltpu.SemaphoreType.DMA((5, 31)),
            pltpu.SemaphoreType.DMA((5, 32)),
            pltpu.SemaphoreType.DMA((5,)),
            pltpu.SemaphoreType.DMA((7,)),
        ],
        compiler_params=pltpu.CompilerParams(
            collective_id=0, has_side_effects=True, vmem_limit_bytes=62 * 1024 * 1024
        ),
        name="forward_layer",
    )(qkv, out, up, down_t, small, x, bounds, lens)


def norm_back(grad, normed, scale, gain):
    wide = grad * gain
    first = jnp.mean(wide, axis=-1, keepdims=True)
    second = jnp.mean(wide * normed, axis=-1, keepdims=True)
    return scale * (wide - first - normed * second)


def middle_kernel(
    rows_i, context, out_cat, up, down, normed_i, scale_i, hidden, active, slope, cot,
    output, grad_one_o, grad_context, small_o, out_g, up_g, down_g,
    two_low, one_low, inner_low, sums,
):
    def tally(at, value):
        sums[at : at + 1, 0 : value.shape[1]] += jnp.sum(value, axis=0, keepdims=True)

    sums[...] = jnp.zeros_like(sums)

    def block(b, carry):
        rows = pl.ds(pl.multiple_of(b * 256, 256), 256)
        normed_one = normed_i[rows, :]
        first = normed_one * row(rows_i, 8) + row(rows_i, 9)
        second = first + mul(active[rows, :], down[...], 1, 1) + row(rows_i, 3)
        normed_two, scale_two = normalize(second)
        output[rows, :] = (normed_two * row(rows_i, 10) + row(rows_i, 11)).astype(BF16)
        grad_out = cot[rows, :].astype(F32)
        grad_two = norm_back(grad_out, normed_two, scale_two, row(rows_i, 10))
        tally(2, grad_out * normed_two)
        tally(3, grad_out)
        tally(5, grad_two)
        low = grad_two.astype(BF16)
        two_low[rows, :] = low
        grad_first = grad_two
        for n in range(4):
            wide = slice(768 * n, 768 * n + 768)
            grad_inner = mul(low, down[:, wide], 1, 0) * slope[rows, wide].astype(F32)
            tally(6 + n, grad_inner)
            part = grad_inner.astype(BF16)
            inner_low[rows, wide] = part
            grad_first = grad_first + mul(part, up[:, wide], 1, 1)
        grad_one = norm_back(grad_first, normed_one, scale_i[rows, 0:1], row(rows_i, 8))
        tally(0, grad_first * normed_one)
        tally(1, grad_first)
        tally(4, grad_one)
        grad_one_o[rows, :] = grad_one
        part = grad_one.astype(BF16)
        one_low[rows, :] = part
        grad_context[:, :, rows] = mul(out_cat[...], part, 1, 1).astype(BF16).reshape(4, 192, 256)
        return carry

    lax.fori_loop(0, 4, block, 0)
    two_t = two_low[...].T
    hidden_t = hidden[...].T
    for n in range(6):
        wide = slice(512 * n, 512 * n + 512)
        down_g[:, wide] = mul(two_t, active[:, wide], 1, 0).astype(BF16)
        up_g[:, wide] = mul(hidden_t, inner_low[:, wide], 1, 0).astype(BF16)
    ctx = context[...].reshape(768, 1024)
    full = mul(ctx, one_low[...], 1, 0).astype(BF16)
    for g in range(4):
        out_g[g] = full[:, 192 * g : 192 * g + 192].reshape(8, 96, 192)
    small_o[...] = sums[...]


def middle(rows, context, out_cat, up, down, normed, scale, hidden, active, slope, cot):
    vmem = pl.BlockSpec(memory_space=pltpu.VMEM)
    t, d = cot.shape
    shape = jax.ShapeDtypeStruct
    return pl.pallas_call(
        middle_kernel,
        out_shape=[
            shape((t, d), BF16),
            shape((t, d), F32),
            shape((4, 192, t), BF16),
            shape((16, d), F32),
            shape(GATHERED[1], BF16),
            shape(GATHERED[2], BF16),
            shape(GATHERED[3], BF16),
        ],
        in_specs=[vmem] * 11,
        out_specs=[vmem] * 7,
        scratch_shapes=[
            pltpu.VMEM((t, d), BF16),
            pltpu.VMEM((t, d), BF16),
            pltpu.VMEM((t, 3072), BF16),
            pltpu.VMEM((16, d), F32),
        ],
        compiler_params=pltpu.CompilerParams(vmem_limit_bytes=63 * 1024 * 1024),
        name="middle_layer",
    )(rows, context, out_cat, up, down, normed, scale, hidden, active, slope, cot)


def backward_kernel(*refs):
    (x, bounds, lens, project, log_total, grad_context, grad_one, sums) = refs[:8]
    qkv_h, out_h, up_h, down_h = refs[8:12]
    outs, grad_input = refs[12:17], refs[17]
    acc = refs[18:23]
    slots = [refs[23 + 5 * i : 28 + 5 * i] for i in range(4)]
    weight, x_t, mask, grads, input_t, send_sem, recv_sem, local_sem = refs[43:]
    s = Reduce(acc, *slots, send_sem, recv_sem)
    z_at, x_at, y, c = s.at
    loads = {
        3: pltpu.make_async_copy(down_h, acc[3], local_sem.at[3]),
        2: pltpu.make_async_copy(up_h, acc[2], local_sem.at[2]),
        1: pltpu.make_async_copy(out_h, acc[1], local_sem.at[1]),
        0: pltpu.make_async_copy(qkv_h, weight, local_sem.at[0]),
    }
    for w in (3, 2, 1, 0):
        loads[w].start()
    meet(*s.at)
    loads[3].wait()
    s.open(3)
    loads[2].wait()
    s.open(2)
    loads[1].wait()
    s.open(1)
    fill_mask(mask, bounds, lens, lax.axis_index("head"))
    x_t[...] = x[...].T
    s.fold(3, 0)
    loads[0].wait()
    ones = jnp.ones((8, 1024), BF16)
    bias_rows = []

    def unit(k, m):
        attend_group_back(group_of(k, y, c), m, project, mask, log_total, grad_context, grads)

    def close_group(k):
        g = group_of(k, y, c)
        got = grads[...]
        acc[0][g] = mul(x_t[...], got, 1, 1).astype(BF16).reshape(8, 96, 576)
        part = mul(weight[g].reshape(768, 576), got, 1, 0)
        if k == 3:
            input_t[...] = part
        else:
            input_t[...] += part
        per_column = mul(ones, got, 1, 1)
        sums_q = jnp.concatenate([per_column[0:1, 192 * j : 192 * j + 64] for j in range(3)], axis=1)
        sums_v = jnp.concatenate(
            [per_column[0:1, 192 * j + 128 : 192 * j + 192] for j in range(3)], axis=1
        )
        return g, sums_q, sums_v

    events = [
        [(2, 0)],
        [(3, 1), (1, 0)],
        [(2, 1)],
        [(3, 2), (1, 1)],
        [(2, 2)],
        [(1, 2)],
        [],
        [],
    ]
    tails = []
    for i, k in enumerate((3, 2, 1, 0)):
        for m in range(2):
            unit(k, m)
            for w, stage in events[2 * i + m]:
                s.fold(w, stage)
        tails.append(close_group(k))
    lay_small(acc[4], sums, tails)
    s.open(0)
    s.open(4)
    s.finish(3, outs[3])
    s.finish(2, outs[2])
    s.finish(1, outs[1])
    for b in range(4):
        rows = slice(256 * b, 256 * b + 256)
        grad_input[rows, :] = grad_one[rows, :] + input_t[:, rows].T
    s.fold(4, 0)
    s.fold(0, 0)
    s.fold(4, 1)
    s.fold(0, 1)
    s.fold(4, 2)
    s.fold(0, 2)
    s.finish(4, outs[4])
    s.finish(0, outs[0])
    for w in range(5):
        s.close(w)


def lay_small(small, sums, tails):
    width = sums.shape[1]
    lane = lax.broadcasted_iota(jnp.int32, (1, width), 1)
    query, value = jnp.zeros((1, width), F32), jnp.zeros((1, width), F32)
    for g, sums_q, sums_v in tails:
        mine = lane // 192 == g
        query = jnp.where(mine, jnp.concatenate([sums_q] * 4, axis=1), query)
        value = jnp.where(mine, jnp.concatenate([sums_v] * 4, axis=1), value)
    tops = [
        (query, value, sums[0:1, :]),
        (sums[4:5, :], sums[5:6, :], sums[1:2, :]),
        (sums[6:7, :], sums[7:8, :], sums[2:3, :]),
        (sums[8:9, :], sums[9:10, :], sums[3:4, :]),
    ]
    for h in range(4):
        for r in range(NZ * NX):
            piece = jnp.concatenate([v[:, 96 * r : 96 * r + 96] for v in tops[h]], axis=0)
            small[h, r] = jnp.zeros((8, 128), F32)
            small[h, r, 0:3, 0:96] = piece


def backward(x, bounds, lens, project, log_total, grad_context, grad_one, sums, qkv, out_g, up_g, down_g):
    vmem, hbm = pl.BlockSpec(memory_space=pltpu.VMEM), pl.BlockSpec(memory_space=pl.ANY)
    smem = pl.BlockSpec(memory_space=pltpu.SMEM)
    t, d = x.shape
    return pl.pallas_call(
        backward_kernel,
        out_shape=[jax.ShapeDtypeStruct(one, F32) for one in SHARD]
        + [jax.ShapeDtypeStruct((t, d), F32)],
        in_specs=[vmem, smem, smem] + [vmem] * 5 + [hbm] * 4,
        out_specs=[vmem] * 6,
        scratch_shapes=[pltpu.VMEM(GATHERED[w], kind_of(w)) for w in range(5)]
        + reduce_scratch()
        + [
            pltpu.VMEM(GATHERED[0], BF16),
            pltpu.VMEM((d, t), BF16),
            pltpu.VMEM((2, 512, 512), F32),
            pltpu.VMEM((576, t), BF16),
            pltpu.VMEM((d, t), F32),
            pltpu.SemaphoreType.DMA((5, 31)),
            pltpu.SemaphoreType.DMA((5, 31)),
            pltpu.SemaphoreType.DMA((5,)),
        ],
        compiler_params=pltpu.CompilerParams(
            collective_id=1, has_side_effects=True, vmem_limit_bytes=63 * 1024 * 1024
        ),
        name="backward_layer",
    )(x, bounds, lens, project, log_total, grad_context, grad_one, sums, qkv, out_g, up_g, down_g)


def shards_fast(
    inputs,
    qkv_weight,
    out_weight,
    up_weight,
    down_weight,
    biases,
    norm_params,
    cotangent,
    boundaries,
    lengths,
):
    micro, seq_per, seq, width = inputs.shape
    small = jnp.concatenate([biases, norm_params], axis=0).astype(F32)
    small = jnp.pad(small, ((0, 5), (0, 32)))
    x = inputs.reshape(micro * seq_per * seq, width)
    cot = cotangent.reshape(x.shape)
    (qkv, out, up, down, rows, project, log_total, context, normed, scale, hidden, active,
     slope) = forward(
        qkv_weight, out_weight, up_weight, down_weight.T, small, x, boundaries, lengths
    )
    output, grad_one, grad_context, sums, out_g, up_g, down_g = middle(
        rows, context, out, up, down, normed, scale, hidden, active, slope, cot
    )
    *own, grad_input = backward(
        x, boundaries, lengths, project, log_total, grad_context, grad_one, sums, qkv, out_g,
        up_g, down_g,
    )
    return (
        output.reshape(inputs.shape),
        grad_input.reshape(inputs.shape),
        own[0],
        own[1],
        own[2],
        own[3].T,
        own[4][:2, :96],
        own[4][2:3, :96],
    )


def solution(mesh):
    tokens = P(None, ("rows", "head"), None, None)
    weight = P("rows", "head")
    small = P("head", "rows")
    per_row = P(None, "rows")
    return jax.shard_map(
        functools.partial(shards, fast=fits(mesh)),
        mesh=mesh,
        in_specs=(tokens, weight, weight, weight, weight, small, small, tokens, per_row, per_row),
        out_specs=(tokens, tokens, weight, weight, weight, weight, small, small),
        check_vma=False,
    )
```
